16 devices in a mesh: dp: 2 (over y, z), sp: 8 (over x, core).
Axes of the slice: x: 4, y: 2, z: 1, core: 2. Of those that a mesh axis runs over, the one named last changes fastest.
The devices are a block of a 4x4x8 slice.
Arguments:
- x: bfloat16 [4096, 5120], P(('dp', 'sp')), parts along dimension 0
- gain: bfloat16 [5120], replicated
- wq: bfloat16 [5120, 5120], replicated
- wk: bfloat16 [5120, 5120], replicated
- wv: bfloat16 [5120, 5120], replicated
- wo: bfloat16 [5120, 5120], replicated
Outputs:
- output: bfloat16 [4096, 5120], P(('dp', 'sp')), parts along dimension 0
There are 2 independent parts. The reference program is written for one: setup_inputs(seed, part) draws one part's arguments, and reference() takes and returns one part's arrays. A program takes and returns all parts, laid end to end along the dimension named above; an argument that names none is the same for every part.
All inputs are finite; a program needn't handle non-finite values.
Results may differ from the reference program's by a relative error of at most 0.012.
Values are sent between devices in bfloat16 or wider.
A program may use at most 768 MiB of HBM per device.

```python
import jax
import jax.numpy as jnp
from jax import lax

ROWS = 2048
D = 5120
HEADS = 40
KV_HEADS = 40
HEAD = 128
THETA = 10000


def setup_inputs(seed: int = 0, part: int = 0) -> dict:
    kx, kn, kq, kk, kv, ko = jax.random.split(jax.random.key(seed), 6)

    def weights(key, rows, columns):
        return jax.random.normal(key, (rows, columns), jnp.float32) * rows**-0.5

    drawn = {
        "x": jax.random.normal(jax.random.fold_in(kx, part), (ROWS, D), jnp.float32),
        "gain": 1 + 0.1 * jax.random.normal(kn, (D,), jnp.float32),
        "wq": 2 * weights(kq, D, HEADS * HEAD),
        "wk": 2 * weights(kk, D, KV_HEADS * HEAD),
        "wv": 4 * weights(kv, D, KV_HEADS * HEAD),
        "wo": weights(ko, HEADS * HEAD, D),
    }
    return {k: v.astype(jnp.bfloat16) for k, v in drawn.items()}


def normed(x, gain):
    wide = x.astype(jnp.float32)
    scale = lax.rsqrt(jnp.mean(wide * wide, -1, keepdims=True) + 1e-6)
    return (wide * scale * gain.astype(jnp.float32)).astype(jnp.bfloat16)


def turned(t, place, theta):
    half = t.shape[-1] // 2
    angle = place.astype(jnp.float32)[:, None] * theta ** (-jnp.arange(half, dtype=jnp.float32) / half)
    cos, sin = jnp.cos(angle)[:, None], jnp.sin(angle)[:, None]
    a, b = t[..., :half].astype(jnp.float32), t[..., half:].astype(jnp.float32)
    return jnp.concatenate([a * cos - b * sin, b * cos + a * sin], -1).astype(jnp.bfloat16)


def matmul(a, w):
    return jnp.dot(a, w, preferred_element_type=jnp.float32).astype(jnp.bfloat16)


def einsum(form, a, b):
    return jnp.einsum(form, a.astype(jnp.float32), b.astype(jnp.float32))


def attention(q, k, v):
    scores = einsum("tgsd,ugd->gstu", q, k) * q.shape[-1] ** -0.5
    token = jnp.arange(q.shape[0])
    scores = jnp.where(token[:, None] >= token, scores, -jnp.inf)
    weights = jax.nn.softmax(scores, -1).astype(jnp.bfloat16)
    return einsum("gstu,ugd->tgsd", weights, v).astype(jnp.bfloat16)


def reference(x, gain, wq, wk, wv, wo):
    a, place = normed(x, gain), jnp.arange(ROWS)
    q = turned(matmul(a, wq).reshape(ROWS, HEADS, HEAD), place, THETA).reshape(ROWS, KV_HEADS, -1, HEAD)
    k = turned(matmul(a, wk).reshape(ROWS, KV_HEADS, HEAD), place, THETA)
    v = matmul(a, wv).reshape(ROWS, KV_HEADS, HEAD)
    seen = attention(q, k, v).reshape(ROWS, HEADS * HEAD)
    return (x.astype(jnp.float32) + jnp.dot(seen, wo, preferred_element_type=jnp.float32)).astype(jnp.bfloat16)
```

```python
import functools

import jax
import jax.numpy as jnp
from jax import lax
from jax.experimental import pallas as pl
from jax.experimental.pallas import tpu as pltpu
from jax.sharding import PartitionSpec as P

HEAD = 128
THETA = 10000
LOG2E = 1.4426950408889634
MESH = pl.DeviceIdType.MESH
LAG_R, LAG_S, LAG_O = 2, 4, 5


def _dot(a, b, ca, cb):
    return lax.dot_general(a, b, (((ca,), (cb,)), ((), ())), preferred_element_type=jnp.float32)


def _kernel(x, wq, wk, wv, wo, gain, cos, sin, y, a_s, w_s, q_s, k_s, v_s, kr, vr, qr, or_s, rr, ob, orc, wo_s, y_s, top_s, mix_s,
            a_send, a_recv, w_sem, wo_sem, x_sem, kv_send, kv_recv, q_send, q_recv, o_send, o_recv, p_send, p_recv, *, own, pairs):
    me = lax.axis_index("sp")
    chip, core = me // 2, me % 2
    partner = chip * 2 + (1 - core)
    mirror = 3 - chip
    beside = chip + 1 - 2 * (chip % 2)
    tokens = 2 * own
    half = own
    d = x.shape[1]
    pw = 2 * HEAD
    e = HEAD**-0.5 * LOG2E

    def device(c):
        return {"sp": c * 2 + core}

    def weight_copy(i, n):
        src = (wk, wv, wq)[n]
        slot = (3 * i + n) % 4
        columns = pl.ds(pl.multiple_of((core * pairs + i) * pw, pw), pw)
        return pltpu.make_async_copy(src.at[:, columns], w_s.at[slot], w_sem.at[slot])

    def out_copy(p, n):
        slot = p % 2
        c = core if n == 0 else 1 - core
        rows = pl.ds(pl.multiple_of((c * pairs + p) * pw, pw), pw)
        return pltpu.make_async_copy(wo.at[rows, :], wo_s.at[slot, n], wo_sem.at[slot, n])

    x_copy = pltpu.make_async_copy(x, wo_s.at[1, 0], x_sem)
    x_copy.start()
    for n in range(3):
        weight_copy(0, n).start()
    for n in range(2):
        out_copy(0, n).start()

    barrier = pltpu.get_barrier_semaphore()
    for s in range(1, 8):
        pl.semaphore_signal(barrier, inc=1, device_id={"sp": (me + s) % 8}, device_id_type=MESH)
    pl.semaphore_wait(barrier, 7)

    x_copy.wait()
    piece = own // 4

    def a_copy(n, c):
        rows = pl.ds(c * own + n * piece, piece)
        return pltpu.make_async_remote_copy(
            src_ref=a_s.at[rows, :], dst_ref=a_s.at[rows, :], send_sem=a_send.at[n], recv_sem=a_recv.at[n],
            device_id={"sp": partner}, device_id_type=MESH)

    for n in range(4):
        def norm(r, _):
            at = n * piece + r * 16
            wide = wo_s[1, 0, pl.ds(at, 16), :].astype(jnp.float32)
            scale = lax.rsqrt(jnp.mean(wide * wide, -1, keepdims=True) + 1e-6)
            a_s[pl.ds(pl.multiple_of(core * own + at, 16), 16), :] = (wide * scale * gain[...]).astype(jnp.bfloat16)
            y_s[pl.ds(at, 16), :] = wide

        lax.fori_loop(0, piece // 16, norm, None)
        a_copy(n, core).start()
    for n in range(4):
        a_copy(n, 1 - core).wait_recv()

    def kv_copy(p, v, n, c):
        src, dst = ((k_s, kr), (v_s, vr))[n]
        return pltpu.make_async_remote_copy(
            src_ref=src.at[v, p], dst_ref=dst.at[v, p], send_sem=kv_send.at[n, v, p], recv_sem=kv_recv.at[n, v, p],
            device_id=device(c), device_id_type=MESH)

    def q_copy(p, v, n, c):
        return pltpu.make_async_remote_copy(
            src_ref=q_s.at[v, p], dst_ref=qr.at[v, p], send_sem=q_send.at[v + 2 * n, p], recv_sem=q_recv.at[v, p],
            device_id=device(c), device_id_type=MESH)

    def o_copy(p, v, slot, c):
        return pltpu.make_async_remote_copy(
            src_ref=or_s.at[v, p], dst_ref=rr.at[slot, p], send_sem=o_send.at[v, p], recv_sem=o_recv.at[slot, p],
            device_id=device(c), device_id_type=MESH)

    def p_copy(p):
        return pltpu.make_async_remote_copy(
            src_ref=ob.at[p, 1 - core], dst_ref=orc.at[p], send_sem=p_send.at[p], recv_sem=p_recv.at[p],
            device_id={"sp": partner}, device_id_type=MESH)

    def send_kv(i, n):
        @pl.when(chip < 2)
        def _():
            kv_copy(i, 0, n, 1 - chip).start()
            kv_copy(i, 1, n, mirror).start()

    def send_q(i):
        @pl.when(chip >= 2)
        def _():
            q_copy(i, 0, 0, mirror).start()

        @pl.when(chip == 3)
        def _():
            q_copy(i, 0, 1, 2).start()

        @pl.when(chip >= 1)
        def _():
            q_copy(i, 1, 0, beside).start()

    def project(i):
        for n in range(3):
            weight_copy(i, n).wait()

            @pl.when(i + 1 < pairs)
            def _():
                weight_copy(i + 1, n).start()

            for m in range(0, tokens, 256):
                rows = slice(m, m + 256)
                t = _dot(a_s[rows, :], w_s[(3 * i + n) % 4], 1, 0).astype(jnp.bfloat16)
                for v in range(2):
                    h = t[:, v * HEAD : (v + 1) * HEAD]
                    if n == 1:
                        v_s[v, i, :, rows] = h.T
                    else:
                        wide = h.astype(jnp.float32)
                        turned = wide * cos[rows, :] + pltpu.roll(wide, HEAD // 2, 1) * sin[rows, :]
                        (k_s if n == 0 else q_s)[v, i, rows, :] = turned.astype(jnp.bfloat16)
            if n:
                send_kv(i, n - 1)
        send_q(i)

    def values(v):
        return jnp.concatenate([v, jnp.ones((8, v.shape[1]), jnp.bfloat16)], axis=0)

    def whole(q, k, v):
        spans = [slice(at, at + 256) for at in range(0, tokens, 256)]
        scores = [_dot(k, q[s, :], 1, 1) for s in spans]
        vt = values(v)
        for s, score in zip(spans, scores):
            old = top_s[0:1, s]
            top = jnp.maximum(old, score.max(axis=0, keepdims=True))
            top_s[0:1, s] = top
            weight = jnp.exp2((score - top) * e).astype(jnp.bfloat16)
            mix_s[:, s] = mix_s[:, s] * jnp.exp2((old - top) * e) + _dot(vt, weight, 1, 0)

    def own_keys(q, k, v):
        vt = values(v)
        spans = [slice(at, at + 256) for at in range(0, tokens, 256)]
        scores = [_dot(k[: s.stop, :], q[s, :], 1, 1) for s in spans]
        for s, score in zip(spans, scores):
            key = lax.broadcasted_iota(jnp.int32, score.shape, 0)
            query = lax.broadcasted_iota(jnp.int32, score.shape, 1) + s.start
            score = jnp.where(key <= query, score, -1e30)
            top = score.max(axis=0, keepdims=True)
            top_s[0:1, s] = top
            weight = jnp.exp2((score - top) * e).astype(jnp.bfloat16)
            mix_s[:, s] = _dot(vt[:, : s.stop], weight, 1, 0)

    def for_others(p):
        for v in range(2):
            has_q = chip <= 2 if v == 0 else chip != 1
            use_own = chip <= 2 if v == 0 else (chip == 0) | (chip == 2)
            use_kv = chip <= 1 if v == 0 else chip >= 2

            @pl.when(has_q)
            def _():
                q_copy(p, v, 0, chip).wait_recv()
                top_s[...] = jnp.full(top_s.shape, -1e30, jnp.float32)
                mix_s[...] = jnp.zeros(mix_s.shape, jnp.float32)

            @pl.when(use_own)
            def _():
                whole(qr[v, p], k_s[v, p], v_s[v, p])

            @pl.when(use_kv)
            def _():
                for n in range(2):
                    kv_copy(p, v, n, chip).wait_recv()
                whole(qr[v, p], kr[v, p], vr[v, p])

            @pl.when(has_q)
            def _():
                total = mix_s[HEAD : HEAD + 1, :]
                or_s[v, p, :HEAD, :] = (mix_s[:HEAD, :] * (1 / total)).astype(jnp.bfloat16)
                level = top_s[0:1, :] * e + jnp.log(total) * LOG2E
                high = level.astype(jnp.bfloat16).astype(jnp.float32)
                rest = level - high
                middle = rest.astype(jnp.bfloat16).astype(jnp.float32)
                low = rest - middle
                or_s[v, p, HEAD:, :] = jnp.concatenate([high, middle, low, jnp.zeros((13, tokens), jnp.float32)], axis=0).astype(jnp.bfloat16)

            if v == 0:
                @pl.when(chip <= 1)
                def _():
                    o_copy(p, 0, 0, mirror).start()

                @pl.when(chip == 2)
                def _():
                    o_copy(p, 0, 2, 3).start()
            else:
                @pl.when(has_q)
                def _():
                    o_copy(p, 1, 1, beside).start()

    def take(p, slot):
        o_copy(p, slot % 2, slot, chip).wait_recv()
        tail = rr[slot, p, HEAD:, :].astype(jnp.float32)
        level = tail[0:1, :] + tail[1:2, :] + tail[2:3, :]
        old = top_s[0:1, :]
        top = jnp.maximum(old, level)
        top_s[0:1, :] = top
        keep, add = jnp.exp2(old - top), jnp.exp2(level - top)
        mix_s[:HEAD, :] = mix_s[:HEAD, :] * keep + rr[slot, p, :HEAD, :].astype(jnp.float32) * add
        mix_s[HEAD:, :] = mix_s[HEAD:, :] * keep + add

    def for_own(p):
        for v in range(2):
            own_keys(q_s[v, p], k_s[v, p], v_s[v, p])

            @pl.when((chip == 1) if v == 0 else (chip >= 2))
            def _():
                whole(q_s[v, p], kr[v, p], vr[v, p])

            top_s[...] = top_s[...] * e
            if v == 0:
                @pl.when(chip >= 2)
                def _():
                    take(p, 0)

                @pl.when(chip == 3)
                def _():
                    take(p, 2)
            else:
                @pl.when(chip >= 1)
                def _():
                    take(p, 1)
            seen = (mix_s[:HEAD, :] * (1 / mix_s[HEAD : HEAD + 1, :])).T.astype(jnp.bfloat16)
            for c in range(2):
                ob[p, c, :, v * HEAD : (v + 1) * HEAD] = seen[c * half : (c + 1) * half, :]
        p_copy(p).start()

    wide = 512

    def project_out(p):
        p_copy(p).wait_recv()
        for n in range(2):
            out_copy(p, n).wait()

        @pl.when(p + 1 < pairs)
        def _():
            for n in range(2):
                out_copy(p + 1, n).start()

        def part(c, _):
            at = pl.ds(pl.multiple_of(c * wide, wide), wide)
            y_s[:, at] += _dot(ob[p, core], wo_s[p % 2, 0, :, at], 1, 0) + _dot(orc[p], wo_s[p % 2, 1, :, at], 1, 0)

        lax.fori_loop(0, d // wide, part, None)

    def step(i, _):
        @pl.when(i < pairs)
        def _():
            project(i)

        @pl.when((i >= LAG_R) & (i < pairs + LAG_R))
        def _():
            for_others(i - LAG_R)

        @pl.when((i >= LAG_S) & (i < pairs + LAG_S))
        def _():
            for_own(i - LAG_S)

        @pl.when(i >= LAG_O)
        def _():
            project_out(i - LAG_O)

    lax.fori_loop(0, pairs + LAG_O, step, None)

    def finish(c, _):
        at = pl.ds(pl.multiple_of(c * wide, wide), wide)
        wo_s[0, 0, :, at] = y_s[:, at].astype(jnp.bfloat16)

    lax.fori_loop(0, d // wide, finish, None)
    y_copy = pltpu.make_async_copy(wo_s.at[0, 0], y, x_sem)
    y_copy.start()

    def drain(p, _):
        @pl.when(chip < 2)
        def _():
            for n in range(2):
                kv_copy(p, 0, n, 1 - chip).wait_send()
                kv_copy(p, 1, n, mirror).wait_send()

        @pl.when(chip >= 2)
        def _():
            q_copy(p, 0, 0, mirror).wait_send()

        @pl.when(chip == 3)
        def _():
            q_copy(p, 0, 1, 2).wait_send()

        @pl.when(chip >= 1)
        def _():
            q_copy(p, 1, 0, beside).wait_send()

        @pl.when(chip <= 2)
        def _():
            o_copy(p, 0, 0, mirror).wait_send()

        @pl.when(chip != 1)
        def _():
            o_copy(p, 1, 1, beside).wait_send()

        p_copy(p).wait_send()

    for n in range(4):
        a_copy(n, core).wait_send()
    lax.fori_loop(0, pairs, drain, None)
    y_copy.wait()


def solution(mesh):
    def step(x, gain, wq, wk, wv, wo):
        own, d = x.shape
        tokens, pairs = 2 * own, wq.shape[1] // (4 * HEAD)
        first = lax.axis_index("sp") // 2 * tokens
        place = first + jnp.arange(tokens)
        h = HEAD // 2
        angle = place.astype(jnp.float32)[:, None] * THETA ** (-jnp.arange(h, dtype=jnp.float32) / h)
        cos, sin = jnp.cos(angle), jnp.sin(angle)
        cos, sin = jnp.concatenate([cos, cos], -1), jnp.concatenate([-sin, sin], -1)
        hbm, vmem = pl.BlockSpec(memory_space=pl.ANY), pl.BlockSpec(memory_space=pltpu.VMEM)
        bf, f32, dma = jnp.bfloat16, jnp.float32, pltpu.SemaphoreType.DMA
        per = (2, pairs, tokens, HEAD)
        back = (pairs, HEAD + 16, tokens)
        return pl.pallas_call(
            functools.partial(_kernel, own=own, pairs=pairs),
            out_shape=jax.ShapeDtypeStruct(x.shape, x.dtype),
            in_specs=[hbm] * 5 + [vmem] * 3,
            out_specs=hbm,
            scratch_shapes=[
                pltpu.VMEM((tokens, d), bf),
                pltpu.VMEM((4, d, 2 * HEAD), bf),
                pltpu.VMEM(per, bf),
                pltpu.VMEM(per, bf),
                pltpu.VMEM((2, pairs, HEAD, tokens), bf),
                pltpu.VMEM(per, bf),
                pltpu.VMEM((2, pairs, HEAD, tokens), bf),
                pltpu.VMEM(per, bf),
                pltpu.VMEM((2, *back), bf),
                pltpu.VMEM((3, *back), bf),
                pltpu.VMEM((pairs, 2, own, 2 * HEAD), bf),
                pltpu.VMEM((pairs, own, 2 * HEAD), bf),
                pltpu.VMEM((2, 2, 2 * HEAD, d), bf),
                pltpu.VMEM((own, d), f32),
                pltpu.VMEM((8, tokens), f32),
                pltpu.VMEM((HEAD + 8, tokens), f32),
                dma((4,)), dma((4,)), dma((4,)), dma((2, 2)), dma,
                dma((2, 2, pairs)), dma((2, 2, pairs)),
                dma((3, pairs)), dma((2, pairs)),
                dma((2, pairs)), dma((3, pairs)),
                dma((pairs,)), dma((pairs,)),
            ],
            compiler_params=pltpu.CompilerParams(collective_id=0, has_side_effects=True, vmem_limit_bytes=67_043_328),
            name="layer",
        )(x, wq, wk, wv, wo, gain.astype(f32)[None], cos, sin)

    tokens, whole = P(("dp", "sp"), None), P(None, None)
    return jax.shard_map(
        step,
        mesh=mesh,
        in_specs=(tokens, P(None), whole, whole, whole, whole),
        out_specs=tokens,
        check_vma=False,
    )
```

```python
import functools

import jax
import jax.numpy as jnp
import numpy as np
from jax import lax
from jax.experimental import pallas as pl
from jax.experimental.pallas import tpu as pltpu
from jax.sharding import PartitionSpec as P

HEAD = 128
THETA = 10000
LOG2E = 1.4426950408889634
MESH = pl.DeviceIdType.MESH
LAG_R, LAG_S, LAG_O = 1, 2, 3


def _dot(a, b, ca, cb):
    return lax.dot_general(a, b, (((ca,), (cb,)), ((), ())), preferred_element_type=jnp.float32)


def _kernel(x, wq, wk, wv, wo, gain, freq, y, a_s, w_s, q_s, k_s, v_s, kr, vr, qr, or_s, rr, ob, orc, wo_s, y_s, cos, sin, gain_s,
            a_send, a_recv, w_sem, wo_sem, x_sem, y_sem, kv_send, kv_recv, q_send, q_recv, o_send, o_recv, p_send, p_recv, *, own, pairs):
    me = lax.axis_index("sp")
    chip, core = me // 2, me % 2
    partner = chip * 2 + (1 - core)
    mirror = 3 - chip
    beside = chip + 1 - 2 * (chip % 2)
    tokens = 2 * own
    d = x.shape[1]
    pw = 2 * HEAD
    e = HEAD**-0.5 * LOG2E

    def device(c):
        return {"sp": c * 2 + core}

    def weight_copy(i, n):
        src = (wk, wv, wq)[n]
        slot = (3 * i + n) % 4
        columns = pl.ds(pl.multiple_of((core * pairs + jnp.minimum(i, pairs - 1)) * pw, pw), pw)
        return pltpu.make_async_copy(src.at[:, columns], w_s.at[slot], w_sem.at[slot])

    def out_copy(p, n):
        slot = p % 2
        c = core if n == 0 else 1 - core
        rows = pl.ds(pl.multiple_of((c * pairs + p) * pw, pw), pw)
        return pltpu.make_async_copy(wo.at[rows, :], wo_s.at[slot, pl.ds(n * pw, pw), :], wo_sem.at[slot, n])

    x_copy = pltpu.make_async_copy(x, wo_s.at[1, pl.ds(0, own), :], x_sem)
    x_copy.start()
    for n in range(3):
        weight_copy(0, n).start()
    for n in range(2):
        out_copy(0, n).start()

    barrier = pltpu.get_barrier_semaphore()
    for s in range(1, 8):
        pl.semaphore_signal(barrier, inc=1, device_id={"sp": (me + s) % 8}, device_id_type=MESH)

    def tables(r, _):
        rows = pl.ds(pl.multiple_of(r * 64, 64), 64)
        place = (chip * tokens + r * 64 + lax.broadcasted_iota(jnp.int32, (64, HEAD), 0)).astype(jnp.float32)
        angle = place * freq[...]
        turn = jnp.sin(angle)
        cos[rows, :] = jnp.cos(angle)
        sin[rows, :] = jnp.where(lax.broadcasted_iota(jnp.int32, (64, HEAD), 1) < HEAD // 2, -turn, turn)

    lax.fori_loop(0, tokens // 64, tables, None)
    for n in range(d // HEAD):
        gain_s[:, n * HEAD : (n + 1) * HEAD] = gain[n : n + 1, :].astype(jnp.float32)
    pl.semaphore_wait(barrier, 7)

    x_copy.wait()
    piece = own // 4

    def a_copy(n, c):
        rows = pl.ds(c * own + n * piece, piece)
        return pltpu.make_async_remote_copy(
            src_ref=a_s.at[rows, :], dst_ref=a_s.at[rows, :], send_sem=a_send.at[n], recv_sem=a_recv.at[n],
            device_id={"sp": partner}, device_id_type=MESH)

    for n in range(4):
        def norm(r, _):
            at = n * piece + r * 32
            wide = wo_s[1, pl.ds(at, 32), :].astype(jnp.float32)
            scale = lax.rsqrt(jnp.mean(wide * wide, -1, keepdims=True) + 1e-6)
            a_s[pl.ds(pl.multiple_of(core * own + at, 32), 32), :] = (wide * scale * gain_s[...]).astype(jnp.bfloat16)
            y_s[pl.ds(at, 32), :] = wide

        lax.fori_loop(0, piece // 32, norm, None)
        a_copy(n, core).start()

    def kv_copy(p, v, n, c):
        src, dst = ((k_s, kr), (v_s, vr))[n]
        return pltpu.make_async_remote_copy(
            src_ref=src.at[v, p], dst_ref=dst.at[v, p], send_sem=kv_send.at[n, v, p], recv_sem=kv_recv.at[n, v, p],
            device_id=device(c), device_id_type=MESH)

    def q_copy(p, v, n, c):
        return pltpu.make_async_remote_copy(
            src_ref=q_s.at[v, p], dst_ref=qr.at[v, p], send_sem=q_send.at[v + 2 * n, p], recv_sem=q_recv.at[v, p],
            device_id=device(c), device_id_type=MESH)

    def o_copy(p, v, slot, c):
        return pltpu.make_async_remote_copy(
            src_ref=or_s.at[v, p], dst_ref=rr.at[slot, p], send_sem=o_send.at[v, p], recv_sem=o_recv.at[slot, p],
            device_id=device(c), device_id_type=MESH)

    def p_copy(p):
        return pltpu.make_async_remote_copy(
            src_ref=ob.at[p, 1 - core], dst_ref=orc.at[p], send_sem=p_send.at[p], recv_sem=p_recv.at[p],
            device_id={"sp": partner}, device_id_type=MESH)

    def send_kv(i, n):
        @pl.when(chip < 2)
        def _():
            kv_copy(i, 0, n, 1 - chip).start()
            kv_copy(i, 1, n, mirror).start()

    def send_q(i):
        @pl.when(chip >= 2)
        def _():
            q_copy(i, 0, 0, mirror).start()

        @pl.when(chip == 3)
        def _():
            q_copy(i, 0, 1, 2).start()

        @pl.when(chip >= 1)
        def _():
            q_copy(i, 1, 0, beside).start()

    def project_rows(i, n, rows):
        t = _dot(a_s[rows, :], w_s[(3 * i + n) % 4], 1, 0).astype(jnp.bfloat16)
        for v in range(2):
            h = t[:, v * HEAD : (v + 1) * HEAD]
            if n == 1:
                v_s[v, i, :, rows] = h.T
            else:
                wide = h.astype(jnp.float32)
                turned = wide * cos[rows, :] + pltpu.roll(wide, HEAD // 2, 1) * sin[rows, :]
                (k_s if n == 0 else q_s)[v, i, rows, :] = turned.astype(jnp.bfloat16)

    def project_first():
        weight_copy(1, 0).start()
        for n in range(3):
            weight_copy(0, n).wait()
            project_rows(0, n, pl.ds(pl.multiple_of(core * own, own), own))
        for m in range(4):
            a_copy(m, 1 - core).wait_recv()
        for n in range(3):
            project_rows(0, n, pl.ds(pl.multiple_of((1 - core) * own, own), own))
            if n < 2:
                weight_copy(1, n + 1).start()
                send_kv(0, n)
            else:
                send_q(0)

    def project(i):
        for n in range(3):
            weight_copy(i, n).wait()
        for n in range(3):
            weight_copy(i + 1, n).start()
            project_rows(i, n, slice(0, tokens))
        send_kv(i, 0)
        send_kv(i, 1)
        send_q(i)

    spans = [slice(at, at + own) for at in range(0, tokens, own)]

    def attend(jobs):
        scores = []
        for q, blocks in jobs:
            for s in spans:
                row = []
                for k, _, diagonal in blocks:
                    score = _dot(k[: s.stop, :] if diagonal else k, q[s, :], 1, 1)
                    if diagonal:
                        key = lax.broadcasted_iota(jnp.int32, score.shape, 0)
                        query = lax.broadcasted_iota(jnp.int32, score.shape, 1) + s.start
                        score = jnp.where(key <= query, score, -1e30)
                    row.append(score)
                scores.append(row)
        ones = jnp.ones((8, tokens), jnp.bfloat16)
        got = []
        for i, row in enumerate(scores):
            blocks = jobs[i // len(spans)][1]
            top = functools.reduce(jnp.maximum, [score.max(axis=0, keepdims=True) for score in row])
            mix = None
            for score, (_, v, _) in zip(row, blocks):
                weight = jnp.exp2((score - top) * e).astype(jnp.bfloat16)
                seen = jnp.concatenate([v, ones], axis=0)[:, : score.shape[0]]
                part = _dot(seen, weight, 1, 0)
                mix = part if mix is None else mix + part
            got.append((top * e, mix))
        return got

    def for_others(p):
        plans = {0: [(0, "ob"), (1, "o")], 1: [(0, "ob")], 2: [(0, "o"), (1, "ob")], 3: [(1, "b")]}
        for c, plan in plans.items():
            @pl.when(chip == c)
            def _():
                jobs = []
                for v, blocks in plan:
                    q_copy(p, v, 0, chip).wait_recv()
                    if "b" in blocks:
                        for n in range(2):
                            kv_copy(p, v, n, chip).wait_recv()
                for v, blocks in plan:
                    where = {"o": (k_s, v_s), "b": (kr, vr)}
                    jobs.append((qr[v, p], [(where[b][0][v, p], where[b][1][v, p], False) for b in blocks]))
                got = attend(jobs)
                parts = []
                for i, (level, mix) in enumerate(got):
                    v, s = plan[i // len(spans)][0], spans[i % len(spans)]
                    total = mix[HEAD : HEAD + 1, :]
                    share = (mix[:HEAD, :] * (1 / total)).astype(jnp.bfloat16)
                    for at in range(0, own, HEAD):
                        or_s[v, p, s.start + at : s.start + at + HEAD, :] = share[:, at : at + HEAD]
                    level = level + jnp.log(total) * LOG2E
                    high = level.astype(jnp.bfloat16).astype(jnp.float32)
                    rest = level - high
                    middle = rest.astype(jnp.bfloat16).astype(jnp.float32)
                    parts += [part[:, at : at + HEAD] for at in range(0, own, HEAD) for part in (high, middle, rest - middle)]
                    if s.stop == tokens:
                        parts += [jnp.zeros((16 - len(parts), HEAD), jnp.float32)]
                        or_s[v, p, tokens:, :] = jnp.concatenate(parts, axis=0).astype(jnp.bfloat16)
                        parts = []
                for v, _ in plan:
                    if v == 0:
                        o_copy(p, 0, 0 if c < 2 else 2, 3 - c if c < 2 else 3).start()
                    else:
                        o_copy(p, 1, 1, beside).start()

    def for_own(p):
        plans = {0: ("", ""), 1: ("b", ""), 2: ("", "b"), 3: ("", "b")}
        back = {0: ((), ()), 1: ((), (1,)), 2: ((0,), (1,)), 3: ((0, 2), (1,))}
        for c, plan in plans.items():
            @pl.when(chip == c)
            def _():
                jobs = []
                for v in range(2):
                    blocks = [(k_s[v, p], v_s[v, p], True)]
                    if plan[v]:
                        blocks.append((kr[v, p], vr[v, p], False))
                    jobs.append((q_s[v, p], blocks))
                got = attend(jobs)
                for v in range(2):
                    for slot in back[c][v]:
                        o_copy(p, v, slot, chip).wait_recv()
                for i, (level, mix) in enumerate(got):
                    v, s = i // len(spans), spans[i % len(spans)]
                    sum_, total = mix[:HEAD, :], mix[HEAD : HEAD + 1, :]
                    rows = range(s.start, s.stop, HEAD)
                    levels = []
                    for slot in back[c][v]:
                        t = rr[slot, p, tokens:, :].astype(jnp.float32)
                        at = [r // HEAD * 3 for r in rows]
                        levels.append(jnp.concatenate([t[n : n + 1, :] + t[n + 1 : n + 2, :] + t[n + 2 : n + 3, :] for n in at], axis=1))
                    if levels:
                        top = functools.reduce(jnp.maximum, levels, level)
                        keep = jnp.exp2(level - top)
                        sum_, total = sum_ * keep, total * keep
                        for slot, there in zip(back[c][v], levels):
                            add = jnp.exp2(there - top)
                            sum_, total = sum_ + jnp.concatenate([rr[slot, p, r : r + HEAD, :] for r in rows], axis=1).astype(jnp.float32) * add, total + add
                    ob[p, i % len(spans), :, v * HEAD : (v + 1) * HEAD] = (sum_ * (1 / total)).T.astype(jnp.bfloat16)
        p_copy(p).start()

    wide, parts = 512, 5

    def y_copy(n):
        at = pl.ds(n * (d // parts), d // parts)
        return pltpu.make_async_copy(wo_s.at[pairs % 2, pl.ds(0, own), at], y.at[:, at], y_sem.at[n])

    def project_out(p):
        p_copy(p).wait_recv()
        for n in range(2):
            out_copy(p, n).wait()

        seen = jnp.concatenate([ob[p, core], orc[p]], axis=1)

        @pl.when(p + 1 < pairs)
        def _():
            for n in range(2):
                out_copy(p + 1, n).start()
            for at in range(0, d, wide):
                y_s[:, at : at + wide] += _dot(seen, wo_s[p % 2, :, at : at + wide], 1, 0)

        @pl.when(p + 1 == pairs)
        def _():
            for n in range(parts):
                for at in range(n * (d // parts), (n + 1) * (d // parts), wide):
                    got = y_s[:, at : at + wide] + _dot(seen, wo_s[(pairs - 1) % 2, :, at : at + wide], 1, 0)
                    wo_s[pairs % 2, :own, at : at + wide] = got.astype(jnp.bfloat16)
                y_copy(n).start()

    def step(i, _):
        @pl.when((i > 0) & (i < pairs))
        def _():
            project(i)

        @pl.when((i >= LAG_R) & (i < pairs + LAG_R))
        def _():
            for_others(i - LAG_R)

        @pl.when((i >= LAG_S) & (i < pairs + LAG_S))
        def _():
            for_own(i - LAG_S)

        @pl.when(i >= LAG_O)
        def _():
            project_out(i - LAG_O)

    project_first()
    lax.fori_loop(1, pairs + LAG_O, step, None)

    for n in range(3):
        weight_copy(pairs, n).wait()

    def drain(p, _):
        @pl.when(chip < 2)
        def _():
            for n in range(2):
                kv_copy(p, 0, n, 1 - chip).wait_send()
                kv_copy(p, 1, n, mirror).wait_send()

        @pl.when(chip >= 2)
        def _():
            q_copy(p, 0, 0, mirror).wait_send()

        @pl.when(chip == 3)
        def _():
            q_copy(p, 0, 1, 2).wait_send()

        @pl.when(chip >= 1)
        def _():
            q_copy(p, 1, 0, beside).wait_send()

        @pl.when(chip <= 2)
        def _():
            o_copy(p, 0, 0, mirror).wait_send()

        @pl.when(chip != 1)
        def _():
            o_copy(p, 1, 1, beside).wait_send()

        p_copy(p).wait_send()

    for n in range(4):
        a_copy(n, core).wait_send()
    lax.fori_loop(0, pairs, drain, None)
    for n in range(parts):
        y_copy(n).wait()


def _move(a, b):
    b[...] = a[...]


def solution(mesh):
    def step(x, gain, wq, wk, wv, wo):
        own, d = x.shape
        tokens, pairs = 2 * own, wq.shape[1] // (4 * HEAD)
        h = HEAD // 2
        freq = jnp.asarray((float(THETA) ** (-(np.arange(HEAD) % h) / h)).astype(np.float32)[None])
        hbm, vmem = pl.BlockSpec(memory_space=pl.ANY), pl.BlockSpec(memory_space=pltpu.VMEM)
        bf, f32, dma = jnp.bfloat16, jnp.float32, pltpu.SemaphoreType.DMA
        per = (2, pairs, tokens, HEAD)
        back = (pairs, tokens + 16, HEAD)
        got = pl.pallas_call(
            functools.partial(_kernel, own=own, pairs=pairs),
            out_shape=jax.ShapeDtypeStruct(x.shape, x.dtype),
            in_specs=[hbm] * 5 + [vmem] * 2,
            out_specs=hbm,
            scratch_shapes=[
                pltpu.VMEM((tokens, d), bf),
                pltpu.VMEM((4, d, 2 * HEAD), bf),
                pltpu.VMEM(per, bf),
                pltpu.VMEM(per, bf),
                pltpu.VMEM((2, pairs, HEAD, tokens), bf),
                pltpu.VMEM(per, bf),
                pltpu.VMEM((2, pairs, HEAD, tokens), bf),
                pltpu.VMEM(per, bf),
                pltpu.VMEM((2, *back), bf),
                pltpu.VMEM((3, *back), bf),
                pltpu.VMEM((pairs, 2, own, 2 * HEAD), bf),
                pltpu.VMEM((pairs, own, 2 * HEAD), bf),
                pltpu.VMEM((2, 4 * HEAD, d), bf),
                pltpu.VMEM((own, d), f32),
                pltpu.VMEM((tokens, HEAD), f32),
                pltpu.VMEM((tokens, HEAD), f32),
                pltpu.VMEM((1, d), f32),
                dma((4,)), dma((4,)), dma((4,)), dma((2, 2)), dma, dma((5,)),
                dma((2, 2, pairs)), dma((2, 2, pairs)),
                dma((3, pairs)), dma((2, pairs)),
                dma((2, pairs)), dma((3, pairs)),
                dma((pairs,)), dma((pairs,)),
            ],
            compiler_params=pltpu.CompilerParams(collective_id=0, has_side_effects=True, vmem_limit_bytes=67_043_328),
            name="layer",
        )(x, wq, wk, wv, wo, gain.reshape(d // HEAD, HEAD), freq)
        block = pl.BlockSpec((own // 4, d), lambda n: (n, 0))
        return pl.pallas_call(
            _move, grid=(4,), in_specs=[block], out_specs=block, out_shape=jax.ShapeDtypeStruct(x.shape, x.dtype), name="move",
            cost_estimate=pl.CostEstimate(flops=0, transcendentals=0, bytes_accessed=4 * x.size),
        )(got)

    tokens, whole = P(("dp", "sp"), None), P(None, None)
    return jax.shard_map(
        step,
        mesh=mesh,
        in_specs=(tokens, P(None), whole, whole, whole, whole),
        out_specs=tokens,
        check_vma=False,
    )
```

```python
import functools

import jax
import jax.numpy as jnp
import numpy as np
from jax import lax
from jax.experimental import pallas as pl
from jax.experimental.pallas import tpu as pltpu
from jax.sharding import PartitionSpec as P

HEAD = 128
THETA = 10000
LOG2E = 1.4426950408889634
MESH = pl.DeviceIdType.MESH
LAG_R, LAG_S, LAG_O = 1, 2, 3


def _dot(a, b, ca, cb):
    return lax.dot_general(a, b, (((ca,), (cb,)), ((), ())), preferred_element_type=jnp.float32)


def _kernel(x, wq, wk, wv, wo, gain, freq, y, a_s, w_s, q_s, k_s, v_s, kr, vr, qr, or_s, rr, ob, orc, wo_s, y_s, cos, sin, gain_s,
            a_send, a_recv, w_sem, wo_sem, x_sem, y_sem, kv_send, kv_recv, q_send, q_recv, o_send, o_recv, p_send, p_recv, *, own, pairs):
    me = lax.axis_index("sp")
    chip, core = me // 2, me % 2
    partner = chip * 2 + (1 - core)
    mirror = 3 - chip
    beside = chip + 1 - 2 * (chip % 2)
    tokens = 2 * own
    d = x.shape[1]
    pw = 2 * HEAD
    e = HEAD**-0.5 * LOG2E

    def device(c):
        return {"sp": c * 2 + core}

    def weight_copy(i, n):
        src = (wk, wv, wq)[n]
        slot = (3 * i + n) % 4
        columns = pl.ds(pl.multiple_of((core * pairs + jnp.minimum(i, pairs - 1)) * pw, pw), pw)
        return pltpu.make_async_copy(src.at[:, columns], w_s.at[slot], w_sem.at[slot])

    def out_copy(p, n):
        slot = p % 2
        c = core if n == 0 else 1 - core
        rows = pl.ds(pl.multiple_of((c * pairs + p) * pw, pw), pw)
        return pltpu.make_async_copy(wo.at[rows, :], wo_s.at[slot, pl.ds(n * pw, pw), :], wo_sem.at[slot, n])

    x_copy = pltpu.make_async_copy(x, wo_s.at[1, pl.ds(0, own), :], x_sem)
    x_copy.start()
    for n in range(3):
        weight_copy(0, n).start()
    for n in range(2):
        out_copy(0, n).start()

    barrier = pltpu.get_barrier_semaphore()
    for s in range(1, 8):
        pl.semaphore_signal(barrier, inc=1, device_id={"sp": (me + s) % 8}, device_id_type=MESH)

    def tables(r, _):
        rows = pl.ds(pl.multiple_of(r * 64, 64), 64)
        place = (chip * tokens + r * 64 + lax.broadcasted_iota(jnp.int32, (64, HEAD), 0)).astype(jnp.float32)
        angle = place * freq[...]
        turn = jnp.sin(angle)
        cos[rows, :] = jnp.cos(angle)
        sin[rows, :] = jnp.where(lax.broadcasted_iota(jnp.int32, (64, HEAD), 1) < HEAD // 2, -turn, turn)

    lax.fori_loop(0, tokens // 64, tables, None)
    for n in range(d // HEAD):
        gain_s[:, n * HEAD : (n + 1) * HEAD] = gain[n : n + 1, :].astype(jnp.float32)
    pl.semaphore_wait(barrier, 7)

    x_copy.wait()
    piece = own // 4

    def a_copy(n, c):
        rows = pl.ds(c * own + n * piece, piece)
        return pltpu.make_async_remote_copy(
            src_ref=a_s.at[rows, :], dst_ref=a_s.at[rows, :], send_sem=a_send.at[n], recv_sem=a_recv.at[n],
            device_id={"sp": partner}, device_id_type=MESH)

    for n in range(4):
        def norm(r, _):
            at = n * piece + r * 32
            wide = wo_s[1, pl.ds(at, 32), :].astype(jnp.float32)
            scale = lax.rsqrt(jnp.mean(wide * wide, -1, keepdims=True) + 1e-6)
            a_s[pl.ds(pl.multiple_of(core * own + at, 32), 32), :] = (wide * scale * gain_s[...]).astype(jnp.bfloat16)
            y_s[pl.ds(at, 32), :] = wide

        lax.fori_loop(0, piece // 32, norm, None)
        a_copy(n, core).start()

    def kv_copy(p, v, n, c):
        src, dst = ((k_s, kr), (v_s, vr))[n]
        return pltpu.make_async_remote_copy(
            src_ref=src.at[v, p], dst_ref=dst.at[v, p], send_sem=kv_send.at[n, v, p], recv_sem=kv_recv.at[n, v, p],
            device_id=device(c), device_id_type=MESH)

    def q_copy(p, v, n, c):
        return pltpu.make_async_remote_copy(
            src_ref=q_s.at[v, p], dst_ref=qr.at[v, p], send_sem=q_send.at[v + 2 * n, p], recv_sem=q_recv.at[v, p],
            device_id=device(c), device_id_type=MESH)

    def o_copy(p, v, slot, c):
        return pltpu.make_async_remote_copy(
            src_ref=or_s.at[v, p], dst_ref=rr.at[slot, p], send_sem=o_send.at[v, p], recv_sem=o_recv.at[slot, p],
            device_id=device(c), device_id_type=MESH)

    def p_copy(p):
        return pltpu.make_async_remote_copy(
            src_ref=ob.at[p, 1 - core], dst_ref=orc.at[p], send_sem=p_send.at[p], recv_sem=p_recv.at[p],
            device_id={"sp": partner}, device_id_type=MESH)

    def send_kv(i, n):
        @pl.when(chip < 2)
        def _():
            kv_copy(i, 0, n, 1 - chip).start()
            kv_copy(i, 1, n, mirror).start()

    def send_q(i):
        @pl.when(chip >= 2)
        def _():
            q_copy(i, 0, 0, mirror).start()

        @pl.when(chip == 3)
        def _():
            q_copy(i, 0, 1, 2).start()

        @pl.when(chip >= 1)
        def _():
            q_copy(i, 1, 0, beside).start()

    def project_rows(i, n, rows):
        t = _dot(a_s[rows, :], w_s[(3 * i + n) % 4], 1, 0).astype(jnp.bfloat16)
        for v in range(2):
            h = t[:, v * HEAD : (v + 1) * HEAD]
            if n == 1:
                v_s[v, i, :, rows] = h.T
            else:
                wide = h.astype(jnp.float32)
                turned = wide * cos[rows, :] + pltpu.roll(wide, HEAD // 2, 1) * sin[rows, :]
                (k_s if n == 0 else q_s)[v, i, rows, :] = turned.astype(jnp.bfloat16)

    def project_first():
        weight_copy(1, 0).start()
        for n in range(3):
            weight_copy(0, n).wait()
            project_rows(0, n, pl.ds(pl.multiple_of(core * own, own), own))
        for m in range(4):
            a_copy(m, 1 - core).wait_recv()
        for n in range(3):
            project_rows(0, n, pl.ds(pl.multiple_of((1 - core) * own, own), own))
            if n < 2:
                weight_copy(1, n + 1).start()
                send_kv(0, n)
            else:
                send_q(0)

    def project(i):
        for n in range(3):
            weight_copy(i, n).wait()
        for n in range(3):
            weight_copy(i + 1, n).start()
            project_rows(i, n, slice(0, tokens))
        send_kv(i, 0)
        send_kv(i, 1)
        send_q(i)

    spans = [slice(at, at + own) for at in range(0, tokens, own)]

    def attend(jobs):
        scores = []
        for q, blocks in jobs:
            for s in spans:
                row = []
                for k, _, diagonal in blocks:
                    score = _dot(k[: s.stop, :] if diagonal else k, q[s, :], 1, 1)
                    if diagonal:
                        key = lax.broadcasted_iota(jnp.int32, score.shape, 0)
                        query = lax.broadcasted_iota(jnp.int32, score.shape, 1) + s.start
                        score = jnp.where(key <= query, score, -1e30)
                    row.append(score)
                scores.append(row)
        ones = jnp.ones((8, tokens), jnp.bfloat16)
        got = []
        for i, row in enumerate(scores):
            blocks = jobs[i // len(spans)][1]
            top = functools.reduce(jnp.maximum, [score.max(axis=0, keepdims=True) for score in row])
            mix = None
            for score, (_, v, _) in zip(row, blocks):
                weight = jnp.exp2((score - top) * e).astype(jnp.bfloat16)
                seen = jnp.concatenate([v, ones], axis=0)[:, : score.shape[0]]
                part = _dot(seen, weight, 1, 0)
                mix = part if mix is None else mix + part
            got.append((top * e, mix))
        return got

    def for_others(p):
        plans = {0: [(0, "ob"), (1, "o")], 1: [(0, "ob")], 2: [(0, "o"), (1, "ob")], 3: [(1, "b")]}
        for c, plan in plans.items():
            @pl.when(chip == c)
            def _():
                jobs = []
                for v, blocks in plan:
                    q_copy(p, v, 0, chip).wait_recv()
                    if "b" in blocks:
                        for n in range(2):
                            kv_copy(p, v, n, chip).wait_recv()
                for v, blocks in plan:
                    where = {"o": (k_s, v_s), "b": (kr, vr)}
                    jobs.append((qr[v, p], [(where[b][0][v, p], where[b][1][v, p], False) for b in blocks]))
                got = attend(jobs)
                parts = []
                for i, (level, mix) in enumerate(got):
                    v, s = plan[i // len(spans)][0], spans[i % len(spans)]
                    total = mix[HEAD : HEAD + 1, :]
                    share = (mix[:HEAD, :] * (1 / total)).astype(jnp.bfloat16)
                    for at in range(0, own, HEAD):
                        or_s[v, p, s.start + at : s.start + at + HEAD, :] = share[:, at : at + HEAD]
                    level = level + jnp.log(total) * LOG2E
                    high = level.astype(jnp.bfloat16).astype(jnp.float32)
                    rest = level - high
                    middle = rest.astype(jnp.bfloat16).astype(jnp.float32)
                    parts += [part[:, at : at + HEAD] for at in range(0, own, HEAD) for part in (high, middle, rest - middle)]
                    if s.stop == tokens:
                        parts += [jnp.zeros((16 - len(parts), HEAD), jnp.float32)]
                        or_s[v, p, tokens:, :] = jnp.concatenate(parts, axis=0).astype(jnp.bfloat16)
                        parts = []
                for v, _ in plan:
                    if v == 0:
                        o_copy(p, 0, 0 if c < 2 else 2, 3 - c if c < 2 else 3).start()
                    else:
                        o_copy(p, 1, 1, beside).start()

    def for_own(p):
        plans = {0: ("", ""), 1: ("b", ""), 2: ("", "b"), 3: ("", "b")}
        back = {0: ((), ()), 1: ((), (1,)), 2: ((0,), (1,)), 3: ((0, 2), (1,))}
        for c, plan in plans.items():
            @pl.when(chip == c)
            def _():
                jobs = []
                for v in range(2):
                    blocks = [(k_s[v, p], v_s[v, p], True)]
                    if plan[v]:
                        blocks.append((kr[v, p], vr[v, p], False))
                    jobs.append((q_s[v, p], blocks))
                got = attend(jobs)
                for v in range(2):
                    for slot in back[c][v]:
                        o_copy(p, v, slot, chip).wait_recv()
                for i, (level, mix) in enumerate(got):
                    v, s = i // len(spans), spans[i % len(spans)]
                    sum_, total = mix[:HEAD, :], mix[HEAD : HEAD + 1, :]
                    rows = range(s.start, s.stop, HEAD)
                    levels = []
                    for slot in back[c][v]:
                        t = rr[slot, p, tokens:, :].astype(jnp.float32)
                        at = [r // HEAD * 3 for r in rows]
                        levels.append(jnp.concatenate([t[n : n + 1, :] + t[n + 1 : n + 2, :] + t[n + 2 : n + 3, :] for n in at], axis=1))
                    if levels:
                        top = functools.reduce(jnp.maximum, levels, level)
                        keep = jnp.exp2(level - top)
                        sum_, total = sum_ * keep, total * keep
                        for slot, there in zip(back[c][v], levels):
                            add = jnp.exp2(there - top)
                            sum_, total = sum_ + jnp.concatenate([rr[slot, p, r : r + HEAD, :] for r in rows], axis=1).astype(jnp.float32) * add, total + add
                    ob[p, i % len(spans), :, v * HEAD : (v + 1) * HEAD] = (sum_ * (1 / total)).T.astype(jnp.bfloat16)
        p_copy(p).start()

    wide, parts = 512, 5

    def y_copy(n):
        at = pl.ds(n * (d // parts), d // parts)
        return pltpu.make_async_copy(wo_s.at[pairs % 2, pl.ds(0, own), at], y.at[:, at], y_sem.at[n])

    def project_out(p):
        p_copy(p).wait_recv()
        for n in range(2):
            out_copy(p, n).wait()

        seen = jnp.concatenate([ob[p, core], orc[p]], axis=1)

        @pl.when(p + 1 < pairs)
        def _():
            for n in range(2):
                out_copy(p + 1, n).start()
            for at in range(0, d, wide):
                y_s[:, at : at + wide] += _dot(seen, wo_s[p % 2, :, at : at + wide], 1, 0)

        @pl.when(p + 1 == pairs)
        def _():
            for n in range(parts):
                for at in range(n * (d // parts), (n + 1) * (d // parts), wide):
                    got = y_s[:, at : at + wide] + _dot(seen, wo_s[(pairs - 1) % 2, :, at : at + wide], 1, 0)
                    wo_s[pairs % 2, :own, at : at + wide] = got.astype(jnp.bfloat16)
                y_copy(n).start()

    def step(i, _):
        @pl.when((i > 0) & (i < pairs))
        def _():
            project(i)

        @pl.when((i >= LAG_O) & (i < pairs + LAG_O))
        def _():
            project_out(i - LAG_O)

        @pl.when((i >= LAG_R) & (i < pairs + LAG_R))
        def _():
            for_others(i - LAG_R)

        @pl.when((i >= LAG_S) & (i < pairs + LAG_S))
        def _():
            for_own(i - LAG_S)

    project_first()
    lax.fori_loop(1, pairs + LAG_O, step, None)

    for n in range(3):
        weight_copy(pairs, n).wait()

    def drain(p, _):
        @pl.when(chip < 2)
        def _():
            for n in range(2):
                kv_copy(p, 0, n, 1 - chip).wait_send()
                kv_copy(p, 1, n, mirror).wait_send()

        @pl.when(chip >= 2)
        def _():
            q_copy(p, 0, 0, mirror).wait_send()

        @pl.when(chip == 3)
        def _():
            q_copy(p, 0, 1, 2).wait_send()

        @pl.when(chip >= 1)
        def _():
            q_copy(p, 1, 0, beside).wait_send()

        @pl.when(chip <= 2)
        def _():
            o_copy(p, 0, 0, mirror).wait_send()

        @pl.when(chip != 1)
        def _():
            o_copy(p, 1, 1, beside).wait_send()

        p_copy(p).wait_send()

    for n in range(4):
        a_copy(n, core).wait_send()
    lax.fori_loop(0, pairs, drain, None)
    for n in range(parts):
        y_copy(n).wait()


def _move(a, b, held, read, written, *, parts):
    rows = a.shape[0] // parts

    def take(n):
        return pltpu.make_async_copy(a.at[pl.ds(n * rows, rows), :], held.at[n], read.at[n])

    def put(n):
        return pltpu.make_async_copy(held.at[n], b.at[pl.ds(n * rows, rows), :], written.at[n])

    for n in range(parts):
        take(n).start()
    for n in range(parts):
        take(n).wait()
        put(n).start()
    for n in range(parts):
        put(n).wait()


def solution(mesh):
    def step(x, gain, wq, wk, wv, wo):
        own, d = x.shape
        tokens, pairs = 2 * own, wq.shape[1] // (4 * HEAD)
        h = HEAD // 2
        freq = jnp.asarray((float(THETA) ** (-(np.arange(HEAD) % h) / h)).astype(np.float32)[None])
        hbm, vmem = pl.BlockSpec(memory_space=pl.ANY), pl.BlockSpec(memory_space=pltpu.VMEM)
        bf, f32, dma = jnp.bfloat16, jnp.float32, pltpu.SemaphoreType.DMA
        per = (2, pairs, tokens, HEAD)
        back = (pairs, tokens + 16, HEAD)
        got = pl.pallas_call(
            functools.partial(_kernel, own=own, pairs=pairs),
            out_shape=jax.ShapeDtypeStruct(x.shape, x.dtype),
            in_specs=[hbm] * 5 + [vmem] * 2,
            out_specs=hbm,
            scratch_shapes=[
                pltpu.VMEM((tokens, d), bf),
                pltpu.VMEM((4, d, 2 * HEAD), bf),
                pltpu.VMEM(per, bf),
                pltpu.VMEM(per, bf),
                pltpu.VMEM((2, pairs, HEAD, tokens), bf),
                pltpu.VMEM(per, bf),
                pltpu.VMEM((2, pairs, HEAD, tokens), bf),
                pltpu.VMEM(per, bf),
                pltpu.VMEM((2, *back), bf),
                pltpu.VMEM((3, *back), bf),
                pltpu.VMEM((pairs, 2, own, 2 * HEAD), bf),
                pltpu.VMEM((pairs, own, 2 * HEAD), bf),
                pltpu.VMEM((2, 4 * HEAD, d), bf),
                pltpu.VMEM((own, d), f32),
                pltpu.VMEM((tokens, HEAD), f32),
                pltpu.VMEM((tokens, HEAD), f32),
                pltpu.VMEM((1, d), f32),
                dma((4,)), dma((4,)), dma((4,)), dma((2, 2)), dma, dma((5,)),
                dma((2, 2, pairs)), dma((2, 2, pairs)),
                dma((3, pairs)), dma((2, pairs)),
                dma((2, pairs)), dma((3, pairs)),
                dma((pairs,)), dma((pairs,)),
            ],
            compiler_params=pltpu.CompilerParams(collective_id=0, has_side_effects=True, vmem_limit_bytes=67_043_328),
            name="layer",
        )(x, wq, wk, wv, wo, gain.reshape(d // HEAD, HEAD), freq)
        return pl.pallas_call(
            functools.partial(_move, parts=8), in_specs=[hbm], out_specs=hbm, out_shape=jax.ShapeDtypeStruct(x.shape, x.dtype), name="move",
            scratch_shapes=[pltpu.VMEM((8, own // 8, d), bf), dma((8,)), dma((8,))],
            cost_estimate=pl.CostEstimate(flops=0, transcendentals=0, bytes_accessed=4 * x.size),
        )(got)

    tokens, whole = P(("dp", "sp"), None), P(None, None)
    return jax.shard_map(
        step,
        mesh=mesh,
        in_specs=(tokens, P(None), whole, whole, whole, whole),
        out_specs=tokens,
        check_vma=False,
    )
```
